32 devices in a mesh: section: 4 (over y, x), expert: 8 (over z, core).
Axes of the slice: x: 2, y: 2, z: 4, core: 2. Of those that a mesh axis runs over, the one named last changes fastest.
Arguments:
- tokens: bfloat16 [8, 64, 2048], P(None, 'expert'), may hold values from -6 to 6
- norm_gain: float32 [2, 2048], replicated, may hold values from 0.1 to 1.9
- w_gate: bfloat16 [4, 2048, 14336], P('section', None, 'expert'), may hold values from -0.125 to 0.125
- w_up: bfloat16 [4, 2048, 14336], P('section', None, 'expert'), may hold values from -0.125 to 0.125
- w_down: bfloat16 [4, 14336, 2048], P('section', 'expert'), may hold values from -0.0625 to 0.0625
- expert_ids: int32 [2, 8, 64, 2], P(None, None, 'expert'), may hold values from 0 to 3, as said below
- slot_ids: int32 [2, 8, 64, 2], P(None, None, 'expert'), may hold values from 0 to 4, as said below
- dropped: int32 [2, 8, 64, 2], P(None, None, 'expert'), may hold values from 0 to 1, as said below
- gate_weights: float32 [2, 8, 64, 2], P(None, None, 'expert'), may hold values from 0.1 to 1
Outputs:
- states: bfloat16 [4, 8, 64, 2048], P('section', None, 'expert')
The draws below stay inside these ranges and needn't reach their ends.
Inputs may be any that keep to these rules, and one draw needn't show every extreme that they name: `expert_ids`: the two experts of a token differ. `slot_ids`: among the kept choices of the tokens of one index of expert that name one expert, the slots are 0, 1, ... up to their count less one, each once. At most 5 kept choices of the tokens of one index of expert name one expert, and a choice is dropped only where 5 kept choices of its index of expert name its expert; in each layer and micro-batch some expert receives exactly 5 kept choices from every index of expert.
All inputs are finite; a program needn't handle non-finite values.
Results may differ from the reference program's by a relative error of at most 0.025.
Values may be sent and summed in bfloat16 or wider, within the bound.
A program may use at most 64 MiB of HBM per device.

```python
import jax
import jax.numpy as jnp
from jax import lax

D = 2048
FF = 7168
EXPERTS = 4
TOK_DEV = 8
MICRO = 8
LOCAL = 2
SHARDS = 4
LAYERS = 2
TOKENS = 64
CAP = 5
N_EXPERT = 8


def routing_draw(key):
    folded = jax.random.fold_in(key, 7)
    subkeys = jax.random.split(folded, 5)
    blocks = LAYERS * MICRO * N_EXPERT
    hot_expert = jax.random.randint(subkeys[4], (LAYERS * MICRO,), 0, EXPERTS)
    hot_expert = jnp.repeat(hot_expert, N_EXPERT)[:, None]
    priority = jax.vmap(lambda subkey: jax.random.permutation(subkey, TOK_DEV))(jax.random.split(subkeys[2], blocks))
    random_pick = jax.random.randint(subkeys[0], (blocks, TOK_DEV), 0, EXPERTS)
    first_pick = jnp.where(priority < CAP, hot_expert, random_pick)
    offset = jax.random.randint(subkeys[1], (blocks, TOK_DEV), 1, EXPERTS)
    second = (first_pick + offset) % EXPERTS
    chosen = jnp.stack([first_pick, second], axis=-1).astype(jnp.int32)
    prio_pair = jnp.stack([priority * 2, priority * 2 + 1], axis=-1).reshape(blocks, 2 * TOK_DEV)
    flat_ids = chosen.reshape(blocks, 2 * TOK_DEV)
    same_expert = flat_ids[:, :, None] == flat_ids[:, None, :]
    earlier = prio_pair[:, None, :] < prio_pair[:, :, None]
    rank_vals = jnp.sum((same_expert & earlier).astype(jnp.int32), axis=-1)
    drop_flag = (rank_vals >= CAP).astype(jnp.int32)
    spare_slot = jax.random.randint(subkeys[3], (blocks, 2 * TOK_DEV), 0, CAP)
    slot_vals = jnp.where(drop_flag == 1, spare_slot, rank_vals).astype(jnp.int32)
    out_shape = (LAYERS, MICRO, TOKENS, 2)
    return (chosen.reshape(out_shape), slot_vals.reshape(out_shape), drop_flag.reshape(out_shape))


def draw_expert_ids(key, part):
    return routing_draw(key)[0]


def draw_slot_ids(key, part):
    return routing_draw(key)[1]


def draw_dropped(key, part):
    return routing_draw(key)[2]


def shard_levels(stream_key, extent, shards, least, high):
    def one(axis_at, shards_of):
        steps = jax.random.uniform(jax.random.fold_in(jax.random.fold_in(stream_key, 6), axis_at), (shards_of,), jnp.float32, least / len(shards), high / len(shards))
        return jnp.repeat(jnp.exp(steps), extent[axis_at] // shards_of).reshape((-1,) + (1,) * (len(extent) - axis_at - 1))

    level = one(*shards[0])
    for cut in shards[1:]:
        level = level * one(*cut)
    return level


def gaussian(rng, dims, deviation, reach, shards=(), held_as=jnp.bfloat16):
    result = deviation * jax.random.normal(rng, dims, jnp.float32)
    if shards:
        result = result * shard_levels(rng, dims, shards, -0.22, 0.18)
    return jnp.clip(result, -reach, reach).astype(held_as)


def setup_inputs(seed: int = 0) -> dict:
    keys = jax.random.split(jax.random.key(seed), 10)
    tokens = gaussian(keys[0], (MICRO, TOKENS, D), 1.0, 6.0, ((1, 8),))
    norm_gain = jnp.clip(1.0 + 0.18 * jax.random.normal(keys[1], (LAYERS, D), jnp.float32), 0.1, 1.9)
    w_gate = gaussian(keys[2], (2 * LAYERS, D, LOCAL * FF), D ** -0.5, 0.125, ((0, 4), (2, 8)))
    w_up = gaussian(keys[3], (2 * LAYERS, D, LOCAL * FF), D ** -0.5, 0.125, ((0, 4), (2, 8)))
    w_down = gaussian(keys[4], (2 * LAYERS, LOCAL * FF, D), FF ** -0.5, 0.0625, ((0, 4), (1, 8)))
    expert_ids = draw_expert_ids(jax.random.fold_in(keys[9], 71), 0)
    slot_ids = draw_slot_ids(jax.random.fold_in(keys[9], 71), 0)
    dropped = draw_dropped(jax.random.fold_in(keys[9], 71), 0)
    gate_weights = jnp.clip(0.1 + 0.9 * jax.random.uniform(keys[8], (LAYERS, MICRO, TOKENS, 2), jnp.float32) ** shard_levels(keys[8], (LAYERS, MICRO, TOKENS, 2), ((2, 8),), -0.2, 0.2), 0.1, 1.0)
    return dict(tokens=tokens, norm_gain=norm_gain, w_gate=w_gate, w_up=w_up, w_down=w_down, expert_ids=expert_ids, slot_ids=slot_ids, dropped=dropped, gate_weights=gate_weights)


def rms_norm(values, gain_row):
    wide_vals = values.astype(jnp.float32)
    inv_scale = lax.rsqrt(lax.optimization_barrier(jnp.mean(wide_vals * wide_vals, axis=-1, keepdims=True)) + 1e-05)
    return (wide_vals * inv_scale * gain_row).astype(jnp.bfloat16)

def expert_output(rows_in, gate_cols, up_cols, down_rows):
    row_count = rows_in.shape[0]
    gate_vals = jnp.dot(rows_in, gate_cols, preferred_element_type=jnp.float32)
    up_vals = jnp.dot(rows_in, up_cols, preferred_element_type=jnp.float32)
    hidden = (jax.nn.silu(gate_vals) * up_vals).astype(jnp.bfloat16)
    pieces = hidden.reshape(row_count, SHARDS, FF // SHARDS).astype(jnp.float32)
    blocks = down_rows.reshape(SHARDS, FF // SHARDS, D).astype(jnp.float32)
    partial_value = jnp.einsum('rsf,sfd->srd', pieces, blocks).astype(jnp.bfloat16)
    partial_value = lax.optimization_barrier(partial_value)
    return lax.optimization_barrier(jnp.sum(partial_value.astype(jnp.float32), axis=0)).astype(jnp.bfloat16)

def reference(tokens, norm_gain, w_gate, w_up, w_down, expert_ids, slot_ids, dropped, gate_weights):
    slot_limit = EXPERTS * N_EXPERT * CAP
    source = (jnp.arange(TOKENS, dtype=jnp.int32) // TOK_DEV)[:, None]
    gate_all = w_gate.reshape(LAYERS, 2, D, LOCAL * FF)
    up_all = w_up.reshape(LAYERS, 2, D, LOCAL * FF)
    down_all = w_down.reshape(LAYERS, 2, LOCAL * FF, D)

    def one_layer(state, layer_args):
        gain_row, gate_pair, up_pair, down_pair, route_all, slot_all, drop_all, weigh_all = layer_args

        def one_micro(pieces):
            current, route_now, slot_now, drop_now, weigh_now = pieces
            normed = rms_norm(current, gain_row)
            target = route_now * (N_EXPERT * CAP) + source * CAP + slot_now
            target = jnp.where(drop_now == 1, slot_limit, target).astype(jnp.int32)
            buffer = jnp.zeros((slot_limit, D), jnp.bfloat16)
            buffer = buffer.at[target[:, 0]].set(normed, mode='drop')
            buffer = buffer.at[target[:, 1]].set(normed, mode='drop')
            grouped = buffer.reshape(EXPERTS, N_EXPERT * CAP, D)
            outputs = []
            for expert_at in range(EXPERTS):
                half_index = expert_at // LOCAL
                inner_index = expert_at % LOCAL
                low = inner_index * FF
                high = (inner_index + 1) * FF
                outputs.append(expert_output(grouped[expert_at], gate_pair[half_index][:, low:high], up_pair[half_index][:, low:high], down_pair[half_index][low:high]))
            produced = jnp.concatenate(outputs, axis=0)
            clipped = jnp.minimum(target, slot_limit - 1).astype(jnp.int32)
            first_half = current.astype(jnp.float32)
            full_mix = current.astype(jnp.float32)
            for member in range(2):
                picked = produced[clipped[:, member]].astype(jnp.float32)
                weighted = weigh_now[:, member:member + 1] * picked
                kept_mask = drop_now[:, member:member + 1] == 0
                first_kept = kept_mask & (route_now[:, member:member + 1] < LOCAL)
                first_half = first_half + jnp.where(first_kept, weighted, 0.0)
                full_mix = full_mix + jnp.where(kept_mask, weighted, 0.0)
            return (first_half.astype(jnp.bfloat16), full_mix.astype(jnp.bfloat16))
        half_state, new_state = lax.map(one_micro, (state, route_all, slot_all, drop_all, weigh_all))
        return (new_state, jnp.stack([half_state, new_state]))
    final_state, paired = lax.scan(one_layer, tokens, (norm_gain, gate_all, up_all, down_all, expert_ids, slot_ids, dropped, gate_weights))
    return paired.reshape(2 * LAYERS, MICRO, TOKENS, D)
```

```python
import jax
import jax.numpy as jnp
from jax import lax
from jax.sharding import PartitionSpec as P


def on_device(tokens, norm_gain, w_gate, w_up, w_down, expert_ids, slot_ids, dropped, gate_weights):
    groups = lax.axis_size("expert")
    sections = lax.axis_size("section")
    section_at = lax.axis_index("section")
    layers = sections // 2
    local_count = 2
    experts = 2 * local_count
    shards = groups // local_count
    micro_count, tok_rows, model_width = tokens.shape
    capacity = 5 * tok_rows // (2 * experts)
    layer_at = section_at // 2
    half_at = section_at % 2
    gate_mat, up_mat, down_mat = w_gate[0], w_up[0], w_down[0]

    def own_layer(value):
        return lax.dynamic_index_in_dim(value, layer_at, 0, keepdims=False)

    gain_row = own_layer(norm_gain)
    local_id = own_layer(expert_ids) - half_at * local_count
    slot = own_layer(slot_ids)
    owned = (own_layer(dropped) == 0) & (local_id >= 0) & (local_id < local_count)
    weigh = own_layer(gate_weights)
    position = jnp.where(owned, local_id * capacity + slot, -1)
    hot = position[..., None] == jnp.arange(local_count * capacity)
    place = jnp.any(hot, axis=2).astype(jnp.bfloat16)
    spread = jnp.sum(jnp.where(hot, weigh[..., None], 0.0), axis=2)

    def expert_rows(received):
        flat = received.reshape(-1, model_width)
        gate_vals = jnp.dot(flat, gate_mat, preferred_element_type=jnp.float32)
        up_vals = jnp.dot(flat, up_mat, preferred_element_type=jnp.float32)
        hidden = (jax.nn.silu(gate_vals) * up_vals).astype(jnp.bfloat16)
        out = jnp.dot(hidden, down_mat, preferred_element_type=jnp.float32).astype(jnp.bfloat16)
        return out.reshape(received.shape)

    current = tokens
    states = jnp.zeros_like(tokens)
    for layer in range(layers):
        mine = layer_at == layer
        wide = current.astype(jnp.float32)
        inv = lax.rsqrt(jnp.mean(wide * wide, axis=-1, keepdims=True) + 1e-05)
        normed = (wide * inv * gain_row).astype(jnp.bfloat16)
        rows = jnp.einsum("mts,mtd->msd", place, normed, preferred_element_type=jnp.float32)
        rows = rows.astype(jnp.bfloat16).reshape(micro_count, local_count, capacity, model_width)
        rows = jnp.transpose(rows, (1, 0, 2, 3)).reshape(local_count, -1, model_width)
        received = lax.all_to_all(jnp.repeat(rows, shards, axis=0), "expert", 0, 0, tiled=True)
        computed = lax.cond(mine, expert_rows, jnp.zeros_like, received)
        returned = lax.all_to_all(computed, "expert", 0, 0, tiled=True)
        summed = jnp.sum(
            returned.astype(jnp.float32).reshape(local_count, shards, micro_count, capacity, model_width), axis=1
        )
        summed = jnp.transpose(summed.astype(jnp.bfloat16), (1, 0, 2, 3)).reshape(micro_count, -1, model_width)
        share = jnp.einsum(
            "mts,msd->mtd", spread, summed.astype(jnp.float32), precision=lax.Precision.HIGHEST
        )
        pairs = [(2 * layer, 2 * layer + 1), (2 * layer + 1, 2 * layer)]
        other = lax.ppermute(share.astype(jnp.bfloat16), "section", pairs)
        full = (wide + share + other.astype(jnp.float32)).astype(jnp.bfloat16)
        half = (wide + share).astype(jnp.bfloat16)
        states = jnp.where(mine, jnp.where(half_at == 0, half, full), states)
        if layer + 1 < layers:
            onward = [(2 * layer + i, 2 * layer + 2 + i) for i in range(2)]
            passed = lax.ppermute(full, "section", onward)
            current = jnp.where(layer_at == layer + 1, passed, current)
    return states[None]


def solution(mesh):
    return jax.shard_map(
        on_device,
        mesh=mesh,
        in_specs=(
            P(None, "expert", None),
            P(),
            P("section", None, "expert"),
            P("section", None, "expert"),
            P("section", "expert", None),
            P(None, None, "expert", None),
            P(None, None, "expert", None),
            P(None, None, "expert", None),
            P(None, None, "expert", None),
        ),
        out_specs=P("section", None, "expert", None),
        check_vma=False,
    )
```

```python
import functools

import jax
import jax.numpy as jnp
from jax import lax
from jax.experimental import pallas as pl
from jax.experimental.pallas import tpu as pltpu
from jax.sharding import PartitionSpec as P

CORES = 2
TILE_ROWS = 16


def kernel(
    groups, layers, chunks, rows,
    tok, gain, pos_row, pos_col, weigh, gate_hbm, up_hbm, down_hbm,
    out,
    gate, up, down, rbuf, sbuf, pbuf, twin, rsum, retbuf, share_out, share_in, fbuf, xin, hid,
    wsem, disp_send, disp_recv, relay_send, twin_send, twin_recv, ret_send, ret_recv,
    share_send, share_recv, x_send, x_recv,
):
    chips = groups // CORES
    per_expert = chips // 2
    model_width = tok.shape[-1]
    width = gate.shape[-1]
    section = lax.axis_index("section")
    me = lax.axis_index("expert")
    layer = section // 2
    half = section % 2
    chip = me // CORES
    core = me % CORES
    sibling = me + 1 - 2 * core
    partner = section + 1 - 2 * half

    def fetch(i):
        src, dst = ((gate_hbm, gate), (up_hbm, up), (down_hbm, down))[i]
        return pltpu.make_async_copy(src.at[0], dst, wsem.at[i])

    def span(index, count=1):
        size = rows * count
        return pl.ds(pl.multiple_of(index * size, TILE_ROWS), size)

    def remote(src, dst, send, recv, **where):
        return pltpu.make_async_remote_copy(
            src_ref=src, dst_ref=dst, send_sem=send, recv_sem=recv,
            device_id=where, device_id_type=pl.DeviceIdType.MESH,
        )

    def chip_at(r):
        return lax.rem(chip + r, chips)

    def direct(c, r):
        there = chip_at(r)
        place = span(core * chips + chip)
        return remote(
            sbuf.at[c, span(there // per_expert)], rbuf.at[c, place], disp_send.at[c, r],
            disp_recv.at[c, core * chips + chip], expert=there * CORES + core,
        )

    def own_rows(c):
        place = core * chips + chip
        return remote(
            sbuf.at[c, span(chip // per_expert)], rbuf.at[c, span(place)], disp_send.at[c, 0],
            disp_recv.at[c, place], expert=sibling,
        )

    def relay(c, r):
        place = core * chips + chip_at(r)
        return remote(
            rbuf.at[c, span(place)], rbuf.at[c, span(place)], relay_send.at[c, r],
            disp_recv.at[c, place], expert=sibling,
        )

    def arrival(c, at_core, at_chip):
        place = at_core * chips + at_chip
        return remote(
            rbuf.at[c, span(place)], rbuf.at[c, span(place)], relay_send.at[c, 0],
            disp_recv.at[c, place], expert=sibling,
        )

    def to_twin(c):
        return remote(
            pbuf.at[c, span(1 - core, chips)], twin.at[c], twin_send.at[c], twin_recv.at[c], expert=sibling
        )

    def giving(c, r):
        there = chip_at(r)
        return remote(
            rsum.at[c, span(there)], retbuf.at[c, span(chip)], ret_send.at[c, r], ret_recv.at[c, chip],
            expert=there * CORES + core,
        )

    def given(c, r):
        there = chip_at(r)
        return remote(
            rsum.at[c, span(there)], retbuf.at[c, span(there)], ret_send.at[c, r], ret_recv.at[c, there],
            expert=there * CORES + core,
        )

    def swap(c):
        return remote(share_out.at[c], share_in.at[c], share_send.at[c], share_recv.at[c], section=partner)

    def hand_on(c):
        return remote(fbuf.at[c], xin.at[c], x_send.at[c], x_recv.at[c], section=lax.rem(section + 2, 2 * layers))

    def dispatch(c):
        current = xin[c].astype(jnp.float32)
        inv = lax.rsqrt(jnp.mean(current * current, axis=-1, keepdims=True) + 1e-05)
        normed = (current * inv * gain[...]).astype(jnp.bfloat16)
        slots = lax.broadcasted_iota(jnp.int32, (2 * rows, tok.shape[1]), 0)
        hot = (slots == pos_row[c, 0:1, :]) | (slots == pos_row[c, 1:2, :])
        place = jnp.where(hot, 1.0, 0.0).astype(jnp.bfloat16)
        sent = jnp.dot(place, normed, preferred_element_type=jnp.float32).astype(jnp.bfloat16)
        sbuf[c] = sent
        own = jnp.where(chip // per_expert == 0, sent[:rows], sent[rows:])
        rbuf[c, span(core * chips + chip), :] = own
        for r in range(chips - 1, 0, -1):
            direct(c, r).start()
        own_rows(c).start()

    def forward(c):
        for r in range(1, chips):
            arrival(c, core, chip_at(r)).wait_recv()
            relay(c, r).start()

    def compute(c):
        for r in range(chips):
            arrival(c, 1 - core, chip_at(r)).wait_recv()
        if c == 0:
            fetch(0).wait()
            fetch(1).wait()
        wide = 256 if width % 256 == 0 else 128

        def inner(t, carry):
            cols = pl.ds(pl.multiple_of(t * wide, wide), wide)
            got = rbuf[c]
            g = jnp.dot(got, gate[:, cols], preferred_element_type=jnp.float32)
            u = jnp.dot(got, up[:, cols], preferred_element_type=jnp.float32)
            hid[:, cols] = (g / (1.0 + jnp.exp(-g)) * u).astype(jnp.bfloat16)
            return carry

        lax.fori_loop(0, width // wide, inner, 0)
        if c == 0:
            fetch(2).wait()

        def outer(t, carry):
            cols = pl.ds(pl.multiple_of(t * 256, 256), 256)
            pbuf[c, :, cols] = jnp.dot(hid[...], down[:, cols], preferred_element_type=jnp.float32).astype(
                jnp.bfloat16
            )
            return carry

        lax.fori_loop(0, model_width // 256, outer, 0)
        to_twin(c).start()

    def pair(c):
        to_twin(c).wait_recv()
        mine = pbuf[c, span(core, chips), :].astype(jnp.float32)
        rsum[c] = (mine + twin[c].astype(jnp.float32)).astype(jnp.bfloat16)
        for r in range(chips - 1, 0, -1):
            giving(c, r).start()
        retbuf[c, span(chip), :] = rsum[c, span(chip), :]

    def combine(c):
        for r in range(1, chips):
            given(c, r).wait_recv()
        parts = []
        for j in range(2):
            total = jnp.zeros((rows, model_width), jnp.float32)
            for i in range(per_expert):
                low = (j * per_expert + i) * rows
                total = total + retbuf[c, low : low + rows, :].astype(jnp.float32)
            parts.append(total)
        made = jnp.concatenate(parts, axis=0)
        slots = lax.broadcasted_iota(jnp.int32, (tok.shape[1], 2 * rows), 1)
        spread = jnp.zeros((tok.shape[1], 2 * rows), jnp.float32)
        for k in range(2):
            spread = spread + jnp.where(slots == pos_col[c, :, k : k + 1], weigh[c, :, k : k + 1], 0.0)
        share = jnp.dot(spread, made, precision=lax.Precision.HIGHEST, preferred_element_type=jnp.float32)
        share_out[c] = share.astype(jnp.bfloat16)
        swap(c).start()
        out[c] = (xin[c].astype(jnp.float32) + share).astype(jnp.bfloat16)

    def finish(c):
        swap(c).wait_recv()
        both = share_out[c].astype(jnp.float32) + share_in[c].astype(jnp.float32)
        full = (xin[c].astype(jnp.float32) + both).astype(jnp.bfloat16)
        fbuf[c] = full

        @pl.when(layer < layers - 1)
        def _():
            hand_on(c).start()

        @pl.when(half == 1)
        def _():
            out[c] = full

    @pl.when(layer == 0)
    def _():
        for c in range(chunks):
            xin[c] = tok[c]
            dispatch(c)

    for i in range(3):
        fetch(i).start()

    def later(c):
        if c < chunks:
            @pl.when(layer > 0)
            def _():
                hand_on(c).wait_recv()
                dispatch(c)

    later(0)
    forward(0)
    for c in range(chunks):
        compute(c)
        pair(c)
        later(c + 1)
        if c + 1 < chunks:
            forward(c + 1)
        if c >= 1:
            finish(c - 1)
        combine(c)
    finish(chunks - 1)

    for c in range(chunks):
        own_rows(c).wait_send()
        to_twin(c).wait_send()
        swap(c).wait_send()
        for r in range(1, chips):
            direct(c, r).wait_send()
            relay(c, r).wait_send()
            giving(c, r).wait_send()

    @pl.when(layer < layers - 1)
    def _():
        for c in range(chunks):
            hand_on(c).wait_send()


def on_device(tokens, norm_gain, w_gate, w_up, w_down, expert_ids, slot_ids, dropped, gate_weights):
    groups = lax.axis_size("expert")
    layers = lax.axis_size("section") // 2
    section_at = lax.axis_index("section")
    local_count = 2
    micro_count, tok_rows, model_width = tokens.shape
    width = w_gate.shape[-1]
    capacity = 5 * tok_rows // (4 * local_count)
    layer_at, half_at = section_at // 2, section_at % 2
    per_chunk = max(1, TILE_ROWS // capacity)
    rows = -(-per_chunk * capacity // TILE_ROWS) * TILE_ROWS
    chunks = -(-micro_count // per_chunk)
    held = per_chunk * tok_rows
    lines = -(-held // TILE_ROWS) * TILE_ROWS
    chips = groups // CORES

    def chunked(value, fill):
        rest = value.shape[2:]
        extra = [(0, chunks * per_chunk - micro_count)] + [(0, 0)] * (value.ndim - 1)
        value = jnp.pad(value, extra, constant_values=fill).reshape((chunks, held) + rest)
        return jnp.pad(value, [(0, 0), (0, lines - held)] + [(0, 0)] * len(rest), constant_values=fill)

    def own_layer(value):
        return lax.dynamic_index_in_dim(value, layer_at, 0, keepdims=False)

    local_id = own_layer(expert_ids) - half_at * local_count
    owned = (own_layer(dropped) == 0) & (local_id >= 0) & (local_id < local_count)
    turn = (jnp.arange(micro_count, dtype=jnp.int32) % per_chunk)[:, None, None]
    position = jnp.where(owned, local_id * rows + turn * capacity + own_layer(slot_ids), -1)
    pos_col = chunked(position, -1)
    pos_row = jnp.transpose(pos_col, (0, 2, 1))
    weigh = chunked(own_layer(gate_weights), 0)
    gain_row = lax.dynamic_slice_in_dim(norm_gain, layer_at, 1, 0)

    vm = pl.BlockSpec(memory_space=pltpu.VMEM)
    hb = pl.BlockSpec(memory_space=pl.ANY)
    half16 = jnp.bfloat16
    dma = pltpu.SemaphoreType.DMA
    made = pl.pallas_call(
        functools.partial(kernel, groups, layers, chunks, rows),
        out_shape=jax.ShapeDtypeStruct((chunks, lines, model_width), half16),
        in_specs=[vm] * 5 + [hb] * 3,
        out_specs=vm,
        scratch_shapes=[
            pltpu.VMEM((model_width, width), half16),
            pltpu.VMEM((model_width, width), half16),
            pltpu.VMEM((width, model_width), half16),
            pltpu.VMEM((chunks, groups * rows, model_width), half16),
            pltpu.VMEM((chunks, 2 * rows, model_width), half16),
            pltpu.VMEM((chunks, groups * rows, model_width), half16),
            pltpu.VMEM((chunks, chips * rows, model_width), half16),
            pltpu.VMEM((chunks, chips * rows, model_width), half16),
            pltpu.VMEM((chunks, chips * rows, model_width), half16),
            pltpu.VMEM((chunks, lines, model_width), half16),
            pltpu.VMEM((chunks, lines, model_width), half16),
            pltpu.VMEM((chunks, lines, model_width), half16),
            pltpu.VMEM((chunks, lines, model_width), half16),
            pltpu.VMEM((groups * rows, width), half16),
            dma((3,)),
            dma((chunks, chips)),
            dma((chunks, groups)),
            dma((chunks, chips)),
            dma((chunks,)),
            dma((chunks,)),
            dma((chunks, chips)),
            dma((chunks, chips)),
            dma((chunks,)),
            dma((chunks,)),
            dma((chunks,)),
            dma((chunks,)),
        ],
        compiler_params=pltpu.CompilerParams(has_side_effects=True, vmem_limit_bytes=58 * 1024 * 1024),
    )(chunked(tokens, 0), gain_row, pos_row, pos_col, weigh, w_gate, w_up, w_down)
    made = made[:, :held].reshape(chunks * per_chunk, tok_rows, model_width)
    return made[None, :micro_count]


def solution(mesh):
    return jax.shard_map(
        on_device,
        mesh=mesh,
        in_specs=(
            P(None, "expert", None),
            P(),
            P("section", None, "expert"),
            P("section", None, "expert"),
            P("section", "expert", None),
            P(None, None, "expert", None),
            P(None, None, "expert", None),
            P(None, None, "expert", None),
            P(None, None, "expert", None),
        ),
        out_specs=P("section", None, "expert", None),
        check_vma=False,
    )
```

```python
import functools

import jax
import jax.numpy as jnp
from jax import lax
from jax.experimental import pallas as pl
from jax.experimental.pallas import tpu as pltpu
from jax.sharding import PartitionSpec as P

CORES = 2
TILE_ROWS = 16


def kernel(
    groups, layers, chunks, rows,
    tok, gain, pos_row, pos_col, weigh, gate_hbm, up_hbm, down_hbm,
    out,
    gate, up, down, rbuf, sbuf, pbuf, twin, rsum, retbuf, share_out, share_in, fbuf, xin, hid,
    wsem, disp_send, disp_recv, relay_send, twin_send, twin_recv, ret_send, ret_recv,
    share_send, share_recv, x_send, x_recv,
):
    chips = groups // CORES
    per_expert = chips // 2
    model_width = tok.shape[-1]
    width = gate.shape[-1]
    section = lax.axis_index("section")
    me = lax.axis_index("expert")
    layer = section // 2
    half = section % 2
    chip = me // CORES
    core = me % CORES
    sibling = me + 1 - 2 * core
    partner = section + 1 - 2 * half

    def fetch(i):
        src, dst = ((gate_hbm, gate), (up_hbm, up), (down_hbm, down))[i]
        return pltpu.make_async_copy(src.at[0], dst, wsem.at[i])

    def span(index, count=1):
        size = rows * count
        return pl.ds(pl.multiple_of(index * size, TILE_ROWS), size)

    def remote(src, dst, send, recv, **where):
        return pltpu.make_async_remote_copy(
            src_ref=src, dst_ref=dst, send_sem=send, recv_sem=recv,
            device_id=where, device_id_type=pl.DeviceIdType.MESH,
        )

    def chip_at(r):
        return lax.rem(chip + r, chips)

    def direct(c, r):
        there = chip_at(r)
        place = span(core * chips + chip)
        return remote(
            sbuf.at[c, span(there // per_expert)], rbuf.at[c, place], disp_send.at[c, r],
            disp_recv.at[c, core * chips + chip], expert=there * CORES + core,
        )

    def own_rows(c):
        place = core * chips + chip
        return remote(
            sbuf.at[c, span(chip // per_expert)], rbuf.at[c, span(place)], disp_send.at[c, 0],
            disp_recv.at[c, place], expert=sibling,
        )

    def relay(c, r):
        place = core * chips + chip_at(r)
        return remote(
            rbuf.at[c, span(place)], rbuf.at[c, span(place)], relay_send.at[c, r],
            disp_recv.at[c, place], expert=sibling,
        )

    def arrival(c, at_core, at_chip):
        place = at_core * chips + at_chip
        return remote(
            rbuf.at[c, span(place)], rbuf.at[c, span(place)], relay_send.at[c, 0],
            disp_recv.at[c, place], expert=sibling,
        )

    def to_twin(c):
        return remote(
            pbuf.at[c, span(1 - core, chips)], twin.at[c], twin_send.at[c], twin_recv.at[c], expert=sibling
        )

    def giving(c, r):
        there = chip_at(r)
        return remote(
            rsum.at[c, span(there)], retbuf.at[c, span(chip)], ret_send.at[c, r], ret_recv.at[c, chip],
            expert=there * CORES + core,
        )

    def given(c, r):
        there = chip_at(r)
        return remote(
            rsum.at[c, span(there)], retbuf.at[c, span(there)], ret_send.at[c, r], ret_recv.at[c, there],
            expert=there * CORES + core,
        )

    def swap(c):
        return remote(share_out.at[c], share_in.at[c], share_send.at[c], share_recv.at[c], section=partner)

    def hand_on(c):
        return remote(fbuf.at[c], xin.at[c], x_send.at[c], x_recv.at[c], section=lax.rem(section + 2, 2 * layers))

    def dispatch(c):
        current = xin[c].astype(jnp.float32)
        inv = lax.rsqrt(jnp.mean(current * current, axis=-1, keepdims=True) + 1e-05)
        normed = (current * inv * gain[...]).astype(jnp.bfloat16)
        slots = lax.broadcasted_iota(jnp.int32, (2 * rows, tok.shape[1]), 0)
        hot = (slots == pos_row[c, 0:1, :]) | (slots == pos_row[c, 1:2, :])
        place = jnp.where(hot, 1.0, 0.0).astype(jnp.bfloat16)
        sent = jnp.dot(place, normed, preferred_element_type=jnp.float32).astype(jnp.bfloat16)
        sbuf[c] = sent
        own = jnp.where(chip // per_expert == 0, sent[:rows], sent[rows:])
        rbuf[c, span(core * chips + chip), :] = own
        for r in range(chips - 1, 0, -1):
            direct(c, r).start()
        own_rows(c).start()

    def forward(c):
        for r in range(1, chips):
            arrival(c, core, chip_at(r)).wait_recv()
            relay(c, r).start()

    def compute(c):
        for r in range(chips):
            arrival(c, 1 - core, chip_at(r)).wait_recv()
        if c == 0:
            fetch(0).wait()
            fetch(1).wait()
        wide = 256 if width % 256 == 0 else 128

        def inner(t, carry):
            cols = pl.ds(pl.multiple_of(t * wide, wide), wide)
            got = rbuf[c]
            g = jnp.dot(got, gate[:, cols], preferred_element_type=jnp.float32)
            u = jnp.dot(got, up[:, cols], preferred_element_type=jnp.float32)
            hid[:, cols] = (g / (1.0 + jnp.exp(-g)) * u).astype(jnp.bfloat16)
            return carry

        lax.fori_loop(0, width // wide, inner, 0, unroll=True)
        if c == 0:
            fetch(2).wait()

        def outer(t, carry):
            cols = pl.ds(pl.multiple_of(t * 512, 512), 512)
            pbuf[c, :, cols] = jnp.dot(hid[...], down[:, cols], preferred_element_type=jnp.float32).astype(
                jnp.bfloat16
            )
            return carry

        lax.fori_loop(0, model_width // 512, outer, 0)
        to_twin(c).start()

    def pair(c):
        to_twin(c).wait_recv()
        mine = pbuf[c, span(core, chips), :].astype(jnp.float32)
        rsum[c] = (mine + twin[c].astype(jnp.float32)).astype(jnp.bfloat16)
        for r in range(chips - 1, 0, -1):
            giving(c, r).start()
        retbuf[c, span(chip), :] = rsum[c, span(chip), :]

    def combine(c):
        for r in range(1, chips):
            given(c, r).wait_recv()
        parts = []
        for j in range(2):
            total = jnp.zeros((rows, model_width), jnp.float32)
            for i in range(per_expert):
                low = (j * per_expert + i) * rows
                total = total + retbuf[c, low : low + rows, :].astype(jnp.float32)
            parts.append(total)
        made = jnp.concatenate(parts, axis=0)
        slots = lax.broadcasted_iota(jnp.int32, (tok.shape[1], 2 * rows), 1)
        spread = jnp.zeros((tok.shape[1], 2 * rows), jnp.float32)
        for k in range(2):
            spread = spread + jnp.where(slots == pos_col[c, :, k : k + 1], weigh[c, :, k : k + 1], 0.0)
        share = jnp.dot(spread, made, precision=lax.Precision.HIGHEST, preferred_element_type=jnp.float32)
        share_out[c] = share.astype(jnp.bfloat16)
        swap(c).start()
        out[c] = (xin[c].astype(jnp.float32) + share).astype(jnp.bfloat16)

    def finish(c):
        swap(c).wait_recv()
        both = share_out[c].astype(jnp.float32) + share_in[c].astype(jnp.float32)
        full = (xin[c].astype(jnp.float32) + both).astype(jnp.bfloat16)
        fbuf[c] = full

        @pl.when(layer < layers - 1)
        def _():
            hand_on(c).start()

        @pl.when(half == 1)
        def _():
            out[c] = full

    def first(c):
        if c < chunks:
            @pl.when(layer == 0)
            def _():
                xin[c] = tok[c]
                dispatch(c)

    def later(c):
        if c < chunks:
            @pl.when(layer > 0)
            def _():
                hand_on(c).wait_recv()
                dispatch(c)

    first(0)
    first(1)
    for i in range(3):
        fetch(i).start()
    later(0)
    forward(0)
    for c in range(chunks):
        compute(c)
        pair(c)
        first(c + 2)
        later(c + 1)
        if c >= 1:
            combine(c - 1)
        if c + 1 < chunks:
            forward(c + 1)
        if c >= 1:
            finish(c - 1)
    combine(chunks - 1)
    finish(chunks - 1)

    for c in range(chunks):
        own_rows(c).wait_send()
        to_twin(c).wait_send()
        swap(c).wait_send()
        for r in range(1, chips):
            direct(c, r).wait_send()
            relay(c, r).wait_send()
            giving(c, r).wait_send()

    @pl.when(layer < layers - 1)
    def _():
        for c in range(chunks):
            hand_on(c).wait_send()


def on_device(tokens, norm_gain, w_gate, w_up, w_down, expert_ids, slot_ids, dropped, gate_weights):
    groups = lax.axis_size("expert")
    layers = lax.axis_size("section") // 2
    section_at = lax.axis_index("section")
    local_count = 2
    micro_count, tok_rows, model_width = tokens.shape
    width = w_gate.shape[-1]
    capacity = 5 * tok_rows // (4 * local_count)
    layer_at, half_at = section_at // 2, section_at % 2
    per_chunk = max(1, TILE_ROWS // capacity)
    rows = -(-per_chunk * capacity // TILE_ROWS) * TILE_ROWS
    chunks = -(-micro_count // per_chunk)
    held = per_chunk * tok_rows
    lines = -(-held // TILE_ROWS) * TILE_ROWS
    chips = groups // CORES

    def chunked(value, fill):
        rest = value.shape[2:]
        extra = [(0, chunks * per_chunk - micro_count)] + [(0, 0)] * (value.ndim - 1)
        value = jnp.pad(value, extra, constant_values=fill).reshape((chunks, held) + rest)
        return jnp.pad(value, [(0, 0), (0, lines - held)] + [(0, 0)] * len(rest), constant_values=fill)

    def own_layer(value):
        return lax.dynamic_index_in_dim(value, layer_at, 0, keepdims=False)

    local_id = own_layer(expert_ids) - half_at * local_count
    owned = (own_layer(dropped) == 0) & (local_id >= 0) & (local_id < local_count)
    turn = (jnp.arange(micro_count, dtype=jnp.int32) % per_chunk)[:, None, None]
    position = jnp.where(owned, local_id * rows + turn * capacity + own_layer(slot_ids), -1)
    pos_col = chunked(position, -1)
    pos_row = jnp.transpose(pos_col, (0, 2, 1))
    weigh = chunked(own_layer(gate_weights), 0)
    gain_row = lax.dynamic_slice_in_dim(norm_gain, layer_at, 1, 0)

    vm = pl.BlockSpec(memory_space=pltpu.VMEM)
    hb = pl.BlockSpec(memory_space=pl.ANY)
    half16 = jnp.bfloat16
    dma = pltpu.SemaphoreType.DMA
    made = pl.pallas_call(
        functools.partial(kernel, groups, layers, chunks, rows),
        out_shape=jax.ShapeDtypeStruct((chunks, lines, model_width), half16),
        in_specs=[vm] * 5 + [hb] * 3,
        out_specs=vm,
        scratch_shapes=[
            pltpu.VMEM((model_width, width), half16),
            pltpu.VMEM((model_width, width), half16),
            pltpu.VMEM((width, model_width), half16),
            pltpu.VMEM((chunks, groups * rows, model_width), half16),
            pltpu.VMEM((chunks, 2 * rows, model_width), half16),
            pltpu.VMEM((chunks, groups * rows, model_width), half16),
            pltpu.VMEM((chunks, chips * rows, model_width), half16),
            pltpu.VMEM((chunks, chips * rows, model_width), half16),
            pltpu.VMEM((chunks, chips * rows, model_width), half16),
            pltpu.VMEM((chunks, lines, model_width), half16),
            pltpu.VMEM((chunks, lines, model_width), half16),
            pltpu.VMEM((chunks, lines, model_width), half16),
            pltpu.VMEM((chunks, lines, model_width), half16),
            pltpu.VMEM((groups * rows, width), half16),
            dma((3,)),
            dma((chunks, chips)),
            dma((chunks, groups)),
            dma((chunks, chips)),
            dma((chunks,)),
            dma((chunks,)),
            dma((chunks, chips)),
            dma((chunks, chips)),
            dma((chunks,)),
            dma((chunks,)),
            dma((chunks,)),
            dma((chunks,)),
        ],
        compiler_params=pltpu.CompilerParams(has_side_effects=True, vmem_limit_bytes=58 * 1024 * 1024),
    )(chunked(tokens, 0), gain_row, pos_row, pos_col, weigh, w_gate, w_up, w_down)
    made = made[:, :held].reshape(chunks * per_chunk, tok_rows, model_width)
    return made[None, :micro_count]


def solution(mesh):
    return jax.shard_map(
        on_device,
        mesh=mesh,
        in_specs=(
            P(None, "expert", None),
            P(),
            P("section", None, "expert"),
            P("section", None, "expert"),
            P("section", "expert", None),
            P(None, None, "expert", None),
            P(None, None, "expert", None),
            P(None, None, "expert", None),
            P(None, None, "expert", None),
        ),
        out_specs=P("section", None, "expert", None),
        check_vma=False,
    )
```
